32 devices in a mesh: seq: 8 (over z, y), fsdp: 4 (over x, core).
Axes of the slice: x: 2, y: 2, z: 4, core: 2. Of those that a mesh axis runs over, the one named last changes fastest.
Arguments:
- queries: bfloat16 [2048, 2048], P('seq', 'fsdp'), may hold values from -2.5 to 2.5
- keys_values: bfloat16 [2048, 512], P('seq', 'fsdp'), may hold values from -2.5 to 2.5
- hidden_in: bfloat16 [2048, 2880], P(('seq', 'fsdp')), may hold values from -6 to 6
- out_weight: bfloat16 [2048, 2880], P('fsdp'), may hold values from -0.5 to 0.5
- norm_gain: float32 [2880], replicated, may hold values from 0.1 to 1.9
- router_weight: bfloat16 [2880, 8], replicated, may hold values from -0.109375 to 0.109375
- expert_ids: int32 [2048, 4], P(('seq', 'fsdp')), may hold values from 0 to 7, all different within a row; in each aligned block of 64 rows (0 to 63, 64 to 127, ...) at most 64 rows name the same one
- expert_gate: bfloat16 [8, 2880, 1536], P('seq', None, 'fsdp'), may hold values from -0.109375 to 0.109375
- expert_up: bfloat16 [8, 2880, 1536], P('seq', None, 'fsdp'), may hold values from -0.109375 to 0.109375
- expert_down: bfloat16 [8, 2880, 1536], P('seq', None, 'fsdp'), may hold values from -0.15625 to 0.15625
Outputs:
- layer_out: bfloat16 [2048, 2880], P(('seq', 'fsdp'))
The draws below stay inside these ranges and needn't reach their ends.
Inputs may be any that keep to these rules, and one draw needn't show every extreme that they name: `expert_ids`: A row names 4 different experts. Within the rows of one device (aligned blocks of 64 rows) no expert is named by more than 64 rows, a bound that some block reaches.
All inputs are finite; a program needn't handle non-finite values.
Results may differ from the reference program's by a relative error of at most 0.0075.
Values may be sent and summed in bfloat16 or wider, within the bound.
A program may use at most 128 MiB of HBM per device.

```python
import math
import jax
import jax.numpy as jnp
import numpy as np
from jax import lax

D = 2880
FF = 1536
HD = 64
QH = 32
KVH = 4
WINDOW = 128
TOPK = 4
TOK_DEV = 256
TOKENS = 2048
ROWS_DEV = 64
EXPERTS = 8
MOST = 64
N_FSDP = 4


def shard_levels(stream_key, dims, shards, smallest, high):
    loudness, own = 1.0, jax.random.fold_in(stream_key, 6)
    for dim, parts in shards:
        heights = jnp.exp(jax.random.uniform(jax.random.fold_in(own, dim), (parts,), jnp.float32, smallest / len(shards), high / len(shards)))
        loudness = loudness * jnp.repeat(heights, dims[dim] // parts).reshape([-1 if axis == dim else 1 for axis in range(len(dims))])
    return loudness


def shared_out(stream_key, own, number, rows, number_of, top, limit, slope):
    ranking = jax.random.permutation(stream_key, number_of)
    packed, ordinary = shares(number_of, rows * top, limit, slope, True), shares(number_of, rows * top, limit, slope, False)
    places = jnp.arange(number_of)

    def named(tallies, offset_by):
        used = int((tallies > 0).sum())
        fixed = max(1, used // 4)
        passed = fixed + (places - fixed + offset_by * (used - fixed)) % max(1, number_of - fixed)
        return jnp.zeros((number_of,), jnp.int32).at[ranking[jnp.where(places < fixed, places, passed)]].set(jnp.asarray(tallies, jnp.int32))

    tallies = jnp.where(number % 4 == 0, named(packed, number // 4), named(ordinary, number - number // 4 - 1))
    mixed = jax.random.permutation(jax.random.fold_in(own, 3), number_of)
    source_of, taker = mixed[0:number_of // 2 * 2:2], mixed[1:number_of // 2 * 2:2]
    slack = jnp.minimum(tallies[source_of] - 1, limit - tallies[taker]) // 2
    slack = jnp.where((source_of == ranking[0]) | (taker == ranking[0]) | (tallies[taker] == 0), 0, jnp.maximum(slack, 0))
    passed = jax.random.randint(jax.random.fold_in(own, 4), (number_of // 2,), 0, 1 << 20) % (slack + 1)
    tallies = tallies.at[source_of].add(-passed).at[taker].add(passed)
    labels = jnp.searchsorted(jnp.cumsum(tallies), jnp.arange(rows * top), side="right").astype(jnp.int32)
    listing = labels.reshape(top, rows).T
    listing = listing[jax.random.permutation(jax.random.fold_in(own, 1), rows)]
    offset_by = jax.random.randint(jax.random.fold_in(own, 2), (rows, 1), 0, top)
    return jnp.take_along_axis(listing, (jnp.arange(top)[None, :] + offset_by) % top, axis=1)


def shares(number_of, total, limit, lean, full):
    portions = [(1 << 20) // math.isqrt(grade ** lean) + 1 for grade in range(1, number_of + 1)]
    largest = limit if full else min(limit, max(-(-total // number_of), total * portions[0] // sum(portions)))
    least = 1 if total - largest >= number_of - 1 else 0
    holding, rest = [largest] + [least] * (number_of - 1), total - largest - least * (number_of - 1)
    while rest > 0:
        candidates = [i for i in range(1, number_of) if holding[i] < largest] or [i for i in range(1, number_of) if holding[i] < limit]
        pool, budget = sum([portions[i] for i in candidates]), rest
        for i in candidates:
            more = min(limit - holding[i], max(1, budget * portions[i] // pool), rest)
            holding[i] = holding[i] + more
            rest = rest - more
    return np.array(holding)


def scatter_about(key, dims, scale, bound, pieces=(), kind=jnp.bfloat16):
    factor_of = shard_levels(key, dims, pieces, -0.22, 0.18) if pieces else 1.0
    drawn = jax.random.normal(key, dims, jnp.float32) * scale * factor_of
    return jnp.minimum(jnp.maximum(drawn, -bound), bound).astype(kind)


def setup_inputs(seed: int = 0) -> dict:
    key_of = jax.random.split(jax.random.key(seed), 11)
    queries = scatter_about(key_of[0], (TOKENS, QH * HD), 1.0, 2.5, ((0, 8), (1, 4)))
    keys_values = scatter_about(key_of[1], (TOKENS, KVH * 2 * HD), 1.0, 2.5, ((0, 8), (1, 4)))
    hidden_in = scatter_about(key_of[2], (TOKENS, D), 1.0, 6.0, ((0, 32),))
    out_weight = scatter_about(key_of[3], (QH * HD, D), (QH * HD // 16) ** -0.5, 0.5, ((0, 4),))
    norm_gain = jnp.clip(1.0 + 0.18 * jax.random.normal(key_of[4], (D,), jnp.float32), 0.1, 1.9)
    router_weight = scatter_about(key_of[5], (D, EXPERTS), D ** -0.5, 0.109375)
    expert_ids_keys = jax.random.split(jax.random.fold_in(key_of[6], 1), TOKENS // ROWS_DEV)
    expert_ids_turns = jax.random.permutation(jax.random.fold_in(key_of[6], 3), TOKENS // ROWS_DEV)
    expert_ids = jax.vmap(lambda own, number: shared_out(jax.random.fold_in(key_of[6], 2), own, number, ROWS_DEV, EXPERTS, TOPK, MOST, 2))(expert_ids_keys, expert_ids_turns).reshape((TOKENS, TOPK))
    expert_gate = scatter_about(key_of[7], (EXPERTS, D, FF), D ** -0.5, 0.109375, ((0, 8), (2, 4)))
    expert_up = scatter_about(key_of[8], (EXPERTS, D, FF), D ** -0.5, 0.109375, ((0, 8), (2, 4)))
    expert_down = scatter_about(key_of[9], (EXPERTS, D, FF), FF ** -0.5, 0.15625, ((0, 8), (2, 4)))
    return dict(queries=queries, keys_values=keys_values, hidden_in=hidden_in, out_weight=out_weight, norm_gain=norm_gain, router_weight=router_weight, expert_ids=expert_ids, expert_gate=expert_gate, expert_up=expert_up, expert_down=expert_down)


def reference(queries, keys_values, hidden_in, out_weight, norm_gain, router_weight, expert_ids, expert_gate, expert_up, expert_down):
    score_scale = 1.0 / math.sqrt(HD)
    groups = QH // KVH
    padded_kv = jnp.concatenate([jnp.zeros((WINDOW, KVH * 2 * HD), keys_values.dtype), keys_values], axis=0)

    def one_block(block_num):
        first_row = block_num * TOK_DEV
        query_rows = lax.dynamic_slice_in_dim(queries, first_row, TOK_DEV, 0).astype(jnp.float32).reshape(TOK_DEV, KVH, groups, HD)
        kv_rows = lax.dynamic_slice_in_dim(padded_kv, first_row, WINDOW + TOK_DEV, 0).astype(jnp.float32).reshape(WINDOW + TOK_DEV, KVH, 2, HD)
        scores = jnp.einsum('tkgd,skd->kgts', query_rows, kv_rows[:, :, 0]) * score_scale
        query_pos = first_row + jnp.arange(TOK_DEV, dtype=jnp.int32)
        key_pos = first_row - WINDOW + jnp.arange(WINDOW + TOK_DEV, dtype=jnp.int32)
        offset = query_pos[:, None] - key_pos[None, :]
        allowed = (offset >= 0) & (offset <= WINDOW) & (key_pos[None, :] >= 0)
        raised = jnp.where(allowed, jnp.exp(scores), 0.0)
        attn_probs = (raised / lax.optimization_barrier(jnp.sum(raised, axis=-1, keepdims=True))).astype(jnp.bfloat16)
        mixed_heads = jnp.einsum('kgts,skd->tkgd', attn_probs.astype(jnp.float32), kv_rows[:, :, 1])
        return mixed_heads.astype(jnp.bfloat16).reshape(TOK_DEV, QH * HD)
    attended = lax.map(one_block, jnp.arange(TOKENS // TOK_DEV, dtype=jnp.int32)).reshape(TOKENS, QH * HD)
    projected = jnp.dot(attended, out_weight, preferred_element_type=jnp.float32)
    stream = (hidden_in.astype(jnp.float32) + projected).astype(jnp.bfloat16)
    stream = lax.optimization_barrier(stream)
    stream_wide = stream.astype(jnp.float32)
    inverse = lax.rsqrt(lax.optimization_barrier(jnp.mean(stream_wide * stream_wide, axis=1, keepdims=True)) + 1e-05)
    normed = (stream_wide * inverse * norm_gain).astype(jnp.bfloat16)
    logits = jnp.dot(normed, router_weight, preferred_element_type=jnp.float32)
    chosen = expert_ids[:, :, None] == jnp.arange(EXPERTS, dtype=jnp.int32)[None, None, :]
    picked = lax.optimization_barrier(jnp.sum(jnp.where(chosen, logits[:, None, :], 0.0), axis=2))
    raised_gates = jnp.exp(picked)
    gates = raised_gates / lax.optimization_barrier(jnp.sum(raised_gates, axis=1, keepdims=True))
    rows_dev = TOK_DEV // N_FSDP
    block_count = TOKENS // rows_dev
    block_ids = expert_ids.reshape(block_count, rows_dev * TOPK)
    onehot = (block_ids[:, :, None] == jnp.arange(EXPERTS, dtype=jnp.int32)[None, None, :]).astype(jnp.int32)
    running = jnp.cumsum(onehot, axis=1, dtype=jnp.int32) - onehot
    slot_ids = lax.optimization_barrier(jnp.sum(running * onehot, axis=2, dtype=jnp.int32))
    block_index = jnp.arange(block_count, dtype=jnp.int32)[:, None]
    assign_index = jnp.arange(rows_dev * TOPK, dtype=jnp.int32)[None, :]
    token_index = block_index * rows_dev + assign_index // TOPK
    position = ((block_ids * block_count + block_index) * MOST + slot_ids).reshape(-1)
    table = jnp.full((EXPERTS * block_count * MOST,), TOKENS, jnp.int32).at[position].set(token_index.reshape(-1).astype(jnp.int32))
    padded_norm = jnp.concatenate([normed, jnp.zeros((1, D), normed.dtype)], axis=0)

    def one_expert(expert_num):
        picks = lax.dynamic_slice_in_dim(table, expert_num * block_count * MOST, block_count * MOST, 0)
        row_block = padded_norm[picks]
        gate_part = jnp.dot(row_block, expert_gate[expert_num], preferred_element_type=jnp.float32)
        up_part = jnp.dot(row_block, expert_up[expert_num], preferred_element_type=jnp.float32)
        hidden = (gate_part * jax.nn.sigmoid(1.702 * gate_part) * (up_part + 1.0)).astype(jnp.bfloat16)
        return jnp.dot(hidden, expert_down[expert_num].T, preferred_element_type=jnp.float32).astype(jnp.bfloat16)
    outputs = lax.map(one_expert, jnp.arange(EXPERTS, dtype=jnp.int32)).reshape(EXPERTS * block_count * MOST, D)
    fetched = outputs[position].astype(jnp.float32).reshape(TOKENS, TOPK, D)
    expert_sum = lax.optimization_barrier(jnp.sum(fetched * gates[:, :, None], axis=1))
    return (stream_wide + expert_sum).astype(jnp.bfloat16)
```

```python
import math

import jax
import jax.numpy as jnp
from jax import lax
from jax.experimental import pallas as pl
from jax.experimental.pallas import tpu as pltpu
from jax.sharding import Mesh, PartitionSpec as P

D = 2880
HD = 64
WINDOW = 128
TOPK = 4


def shifted(shard, axis, by):
    count = lax.axis_size(axis)
    pairs = [(i, i + by) for i in range(count) if 0 <= i + by < count]
    return lax.ppermute(shard, axis, pairs)


def swiglu_piece(row_block, gate_part, up_part):
    gate_vals = jnp.dot(row_block, gate_part, preferred_element_type=jnp.float32)
    up_vals = jnp.dot(row_block, up_part, preferred_element_type=jnp.float32)
    return (gate_vals * jax.nn.sigmoid(1.702 * gate_vals) * (up_vals + 1.0)).astype(jnp.bfloat16)


def down_piece(hidden, down_part):
    return jnp.einsum("nk,dk->nd", hidden, down_part, preferred_element_type=jnp.float32)


def expert_rows(row_block, gate_part, up_part, down_part):
    hidden = swiglu_piece(
        row_block,
        lax.all_gather(gate_part, "fsdp", axis=1, tiled=True),
        lax.all_gather(up_part, "fsdp", axis=1, tiled=True),
    )
    combined = down_piece(hidden, lax.all_gather(down_part, "fsdp", axis=1, tiled=True))
    return combined.astype(jnp.bfloat16)


def per_device(
    queries,
    keys_values,
    hidden_in,
    out_weight,
    norm_gain,
    router_weight,
    expert_ids,
    expert_gate,
    expert_up,
    expert_down,
):
    tok_dev = queries.shape[0]
    kv_heads = keys_values.shape[1] // (2 * HD)
    heads_local = queries.shape[1] // HD
    groups = heads_local // kv_heads
    key_rim = shifted(keys_values[tok_dev - WINDOW :], "seq", 1)
    extended = jnp.concatenate([key_rim, keys_values], axis=0).reshape(
        WINDOW + tok_dev, kv_heads, 2, HD
    )
    grouped = queries.reshape(tok_dev, kv_heads, groups, HD)
    scores = jnp.einsum(
        "tkgd,skd->kgts", grouped, extended[:, :, 0], preferred_element_type=jnp.float32
    ) * (1.0 / math.sqrt(HD))
    first_pos = lax.axis_index("seq") * tok_dev
    query_pos = first_pos + jnp.arange(tok_dev, dtype=jnp.int32)
    key_pos = first_pos - WINDOW + jnp.arange(WINDOW + tok_dev, dtype=jnp.int32)
    offset = query_pos[:, None] - key_pos[None, :]
    allowed = (offset >= 0) & (offset <= WINDOW) & (key_pos[None, :] >= 0)
    raised = jnp.where(allowed, jnp.exp(scores), 0.0)
    attn_probs = (raised / jnp.sum(raised, axis=-1, keepdims=True)).astype(jnp.bfloat16)
    mixed_heads = jnp.einsum(
        "kgts,skd->tkgd", attn_probs, extended[:, :, 1], preferred_element_type=jnp.float32
    )
    attended = mixed_heads.astype(jnp.bfloat16).reshape(tok_dev, heads_local * HD)
    partial_value = jnp.dot(attended, out_weight, preferred_element_type=jnp.float32)
    rows_dev = tok_dev // lax.axis_size("fsdp")
    projected = lax.psum_scatter(partial_value, "fsdp", scatter_dimension=0, tiled=True)
    stream = (hidden_in.astype(jnp.float32) + projected).astype(jnp.bfloat16)
    stream = lax.optimization_barrier(stream)
    stream_wide = stream.astype(jnp.float32)
    inverse = lax.rsqrt(jnp.mean(stream_wide * stream_wide, axis=1, keepdims=True) + 1e-05)
    normed = (stream_wide * inverse * norm_gain).astype(jnp.bfloat16)
    experts = router_weight.shape[1]
    logits = jnp.dot(normed, router_weight, preferred_element_type=jnp.float32)
    chosen = expert_ids[:, :, None] == jnp.arange(experts, dtype=jnp.int32)[None, None, :]
    picked = jnp.sum(jnp.where(chosen, logits[:, None, :], 0.0), axis=2)
    raised_gates = jnp.exp(picked)
    gates = raised_gates / jnp.sum(raised_gates, axis=1, keepdims=True)
    flat_ids = expert_ids.reshape(-1)
    onehot = (flat_ids[:, None] == jnp.arange(experts, dtype=jnp.int32)[None, :]).astype(jnp.int32)
    running = jnp.cumsum(onehot, axis=0, dtype=jnp.int32) - onehot
    slot_ids = jnp.sum(running * onehot, axis=1, dtype=jnp.int32)
    capacity = 2 * tok_dev * TOPK // (lax.axis_size("fsdp") * experts)
    sources = jnp.repeat(normed, TOPK, axis=0)
    outgoing = jnp.zeros((experts, capacity, D), jnp.bfloat16).at[flat_ids, slot_ids].set(sources)
    owners = lax.axis_size("seq")
    per_owner = experts // owners
    outgoing = outgoing.reshape(owners, per_owner, capacity, D)
    received = lax.all_to_all(outgoing, "seq", split_axis=0, concat_axis=0, tiled=True)
    items_now = received.shape[2]
    row_block = received[:, 0].reshape(owners * items_now, D)
    answer = expert_rows(row_block, expert_gate[0], expert_up[0], expert_down[0])
    results = [answer.reshape(owners, items_now, D)]
    processed = jnp.stack(results, axis=1)
    returned = lax.all_to_all(processed, "seq", split_axis=0, concat_axis=0, tiled=True)
    return_table = returned.reshape(experts * capacity, D)
    fetched = (
        return_table[flat_ids * capacity + slot_ids].astype(jnp.float32).reshape(rows_dev, TOPK, D)
    )
    expert_sum = jnp.sum(fetched * gates[:, :, None], axis=1)
    return (stream_wide + expert_sum).astype(jnp.bfloat16)


def attention_partial(queries, keys_values, out_weight):
    tok_dev = queries.shape[0]
    kv_heads = keys_values.shape[1] // (2 * HD)
    heads_local = queries.shape[1] // HD
    groups = heads_local // kv_heads
    key_rim = shifted(keys_values[tok_dev - WINDOW :], "seq", 1)
    extended = jnp.concatenate([key_rim, keys_values], axis=0).reshape(
        WINDOW + tok_dev, kv_heads, 2, HD
    )
    grouped = queries.reshape(tok_dev, kv_heads, groups, HD)
    scores = jnp.einsum(
        "tkgd,skd->kgts", grouped, extended[:, :, 0], preferred_element_type=jnp.float32
    ) * (1.0 / math.sqrt(HD))
    first_pos = lax.axis_index("seq") * tok_dev
    query_pos = first_pos + jnp.arange(tok_dev, dtype=jnp.int32)
    key_pos = first_pos - WINDOW + jnp.arange(WINDOW + tok_dev, dtype=jnp.int32)
    offset = query_pos[:, None] - key_pos[None, :]
    allowed = (offset >= 0) & (offset <= WINDOW) & (key_pos[None, :] >= 0)
    raised = jnp.where(allowed, jnp.exp(scores), 0.0)
    attn_probs = (raised / jnp.sum(raised, axis=-1, keepdims=True)).astype(jnp.bfloat16)
    mixed_heads = jnp.einsum(
        "kgts,skd->tkgd", attn_probs, extended[:, :, 1], preferred_element_type=jnp.float32
    )
    attended = mixed_heads.astype(jnp.bfloat16).reshape(tok_dev, heads_local * HD)
    return jnp.dot(attended, out_weight, preferred_element_type=jnp.float32)


def swapped(value, axis):
    return lax.ppermute(value, axis, [(0, 1), (1, 0)])


MESH = pl.DeviceIdType.MESH


def places():
    seq, far, pair = lax.axis_index("seq"), lax.axis_index("far"), lax.axis_index("pair")
    deep = lax.axis_size("seq") // 2
    return seq // 2, seq % 2, far, pair, deep


def greet(partners):
    barrier = pltpu.get_barrier_semaphore()
    for partner in partners:
        pl.semaphore_signal(barrier, inc=1, device_id=partner, device_id_type=MESH)
    pl.semaphore_wait(barrier, len(partners))


def remote(src, dst, sems, pos, partner):
    return pltpu.make_async_remote_copy(
        src_ref=src,
        dst_ref=dst,
        send_sem=sems.at[0, pos],
        recv_sem=sems.at[1, pos],
        device_id=partner,
        device_id_type=MESH,
    )


def gather_kernel(in_ref, out_ref, held, z_sem, side_sem, relay_sem, own_sem):
    z, y, x, c, deep = places()
    half = in_ref.shape[0] // 2
    y_dev, x_dev = (2 * z + 1 - y, x, c), (2 * z + y, 1 - x, c)
    z_devs = [(2 * ((z + k) % deep) + y, x, c) for k in range(1, deep)]
    greet([y_dev, x_dev, *z_devs])

    def slot(zz, yy, xx):
        return (zz * 2 + yy) * 2 + xx

    mine = slot(z, y, x)
    sent = []
    for k in range(1, deep):
        copy = remote(in_ref, held.at[mine], z_sem, k - 1, z_devs[k - 1])
        copy.start()
        sent.append(copy)
    local = pltpu.make_async_copy(in_ref, held.at[mine], own_sem)
    local.start()

    def relay(k):
        zz = (z + deep - k) % deep
        from_y, from_x = slot(zz, 1 - y, x), slot(zz, y, 1 - x)
        remote(held.at[from_y], held.at[from_y], side_sem, 2 * k, y_dev).wait_recv()
        rows = held.at[from_y, pl.ds(0, half)]
        copy = remote(rows, rows, relay_sem, 2 * k, x_dev)
        copy.start()
        sent.append(copy)
        remote(held.at[from_x], held.at[from_x], side_sem, 2 * k + 1, x_dev).wait_recv()
        rows = held.at[from_x, pl.ds(half, half)]
        copy = remote(rows, rows, relay_sem, 2 * k + 1, y_dev)
        copy.start()
        sent.append(copy)

    for k in range(deep):
        here = slot((z + deep - k) % deep, y, x)
        if k > 0:
            remote(held.at[here], held.at[here], z_sem, k - 1, y_dev).wait_recv()
        src = in_ref if k == 0 else held.at[here]
        for side, partner in ((0, y_dev), (1, x_dev)):
            copy = remote(src, held.at[here], side_sem, 2 * k + side, partner)
            copy.start()
            sent.append(copy)
        if k > 0:
            relay(k - 1)
    relay(deep - 1)
    local.wait()
    for k in range(deep):
        zz = (z + deep - k) % deep
        opposite = slot(zz, 1 - y, 1 - x)
        rows = held.at[opposite, pl.ds(0, half)]
        remote(rows, rows, relay_sem, 2 * k, x_dev).wait_recv()
        rows = held.at[opposite, pl.ds(half, half)]
        remote(rows, rows, relay_sem, 2 * k + 1, y_dev).wait_recv()
    final = pltpu.make_async_copy(held, out_ref, own_sem)
    final.start()
    for copy in sent:
        copy.wait_send()
    final.wait()


def gather_rows(packet):
    deep = lax.axis_size("seq") // 2
    count = 4 * deep
    return pl.pallas_call(
        gather_kernel,
        out_shape=jax.ShapeDtypeStruct((count, *packet.shape), packet.dtype),
        in_specs=[pl.BlockSpec(memory_space=pltpu.VMEM)],
        out_specs=pl.BlockSpec(memory_space=pl.ANY),
        scratch_shapes=[
            pltpu.VMEM((count, *packet.shape), packet.dtype),
            pltpu.SemaphoreType.DMA((2, deep - 1)),
            pltpu.SemaphoreType.DMA((2, 2 * deep)),
            pltpu.SemaphoreType.DMA((2, 2 * deep)),
            pltpu.SemaphoreType.DMA,
        ],
        compiler_params=pltpu.CompilerParams(collective_id=0, has_side_effects=True),
    )(packet)


def scatter_kernel(
    in_ref, out_ref, first, second, staged, lined, arrived, f_sem, s_sem, d_sem, z_sem
):
    z, y, x, c, deep = places()
    half = in_ref.shape[1] // 2
    y_dev, x_dev = (2 * z + 1 - y, x, c), (2 * z + y, 1 - x, c)
    z_devs = [(2 * ((z + k) % deep) + y, x, c) for k in range(1, deep)]
    greet([y_dev, x_dev, *z_devs])
    low, high = pl.ds(0, half), pl.ds(half, half)

    def slot(k, yy, xx):
        return (((z + k) % deep) * 2 + yy) * 2 + xx

    def wide(value):
        return value.astype(jnp.float32)

    order = [*range(1, deep), 0]
    sent = []

    def send(*parts):
        copy = remote(*parts)
        copy.start()
        sent.append(copy)

    for k in order:
        across = slot(k, 1 - y, 1 - x)
        send(in_ref.at[across, low], first.at[k, 0], f_sem, 2 * k, x_dev)
        send(in_ref.at[across, high], first.at[k, 1], f_sem, 2 * k + 1, y_dev)
        to_y, to_x = slot(k, 1 - y, x), slot(k, y, 1 - x)
        send(in_ref.at[to_y, high], second.at[k, 0, high], d_sem, 2 * k, y_dev)
        send(in_ref.at[to_x, low], second.at[k, 1, low], d_sem, 2 * k + 1, x_dev)

    def middle(k):
        to_y, to_x = slot(k, 1 - y, x), slot(k, y, 1 - x)
        remote(first.at[k, 0], first.at[k, 0], f_sem, 2 * k, x_dev).wait_recv()
        staged[k, 0] = (wide(in_ref[to_y, low]) + wide(first[k, 0])).astype(staged.dtype)
        send(staged.at[k, 0], second.at[k, 0, low], s_sem, 2 * k, y_dev)
        remote(first.at[k, 1], first.at[k, 1], f_sem, 2 * k + 1, y_dev).wait_recv()
        staged[k, 1] = (wide(in_ref[to_x, high]) + wide(first[k, 1])).astype(staged.dtype)
        send(staged.at[k, 1], second.at[k, 1, high], s_sem, 2 * k + 1, x_dev)

    def last(k):
        for side, part, sem, partner in (
            (0, low, s_sem, y_dev),
            (0, high, d_sem, y_dev),
            (1, high, s_sem, x_dev),
            (1, low, d_sem, x_dev),
        ):
            ref = second.at[k, side, part]
            remote(ref, ref, sem, 2 * k + side, partner).wait_recv()
        total = wide(in_ref[slot(k, y, x)]) + wide(second[k, 0]) + wide(second[k, 1])
        if k == 0:
            out_ref[...] = total
        else:
            lined[k - 1] = total.astype(lined.dtype)
            send(lined.at[k - 1], arrived.at[k - 1], z_sem, k - 1, z_devs[k - 1])

    for pos in range(deep + 1):
        if pos < deep:
            middle(order[pos])
        if pos > 0:
            last(order[pos - 1])
    for k in range(1, deep):
        remote(arrived.at[k - 1], arrived.at[k - 1], z_sem, k - 1, z_devs[k - 1]).wait_recv()
        out_ref[...] += wide(arrived[k - 1])
    for copy in sent:
        copy.wait_send()


def scatter_rows(answer):
    deep = lax.axis_size("seq") // 2
    _, rows, width = answer.shape
    kind = answer.dtype
    return pl.pallas_call(
        scatter_kernel,
        out_shape=jax.ShapeDtypeStruct((rows, width), jnp.float32),
        in_specs=[pl.BlockSpec(memory_space=pltpu.VMEM)],
        out_specs=pl.BlockSpec(memory_space=pltpu.VMEM),
        scratch_shapes=[
            pltpu.VMEM((deep, 2, rows // 2, width), kind),
            pltpu.VMEM((deep, 2, rows, width), kind),
            pltpu.VMEM((deep, 2, rows // 2, width), kind),
            pltpu.VMEM((deep - 1, rows, width), kind),
            pltpu.VMEM((deep - 1, rows, width), kind),
            pltpu.SemaphoreType.DMA((2, 2 * deep)),
            pltpu.SemaphoreType.DMA((2, 2 * deep)),
            pltpu.SemaphoreType.DMA((2, 2 * deep)),
            pltpu.SemaphoreType.DMA((2, deep - 1)),
        ],
        compiler_params=pltpu.CompilerParams(collective_id=1, has_side_effects=True),
    )(answer)


def dense_device(
    queries,
    keys_values,
    hidden_in,
    out_weight,
    norm_gain,
    router_weight,
    expert_ids,
    expert_gate,
    expert_up,
    expert_down,
):
    gates_w = (expert_gate[0], swapped(expert_gate[0], "pair"))
    ups_w = (expert_up[0], swapped(expert_up[0], "pair"))
    downs_w = (expert_down[0], swapped(expert_down[0], "pair"))
    partial_value = attention_partial(queries, keys_values, out_weight)
    rows = hidden_in.shape[0]
    model = hidden_in.shape[1]
    pair, far = lax.axis_index("pair"), lax.axis_index("far")
    split = partial_value.reshape(2, 2, rows, model)
    mine = jnp.where(pair == 0, split[:, 0], split[:, 1])
    other = jnp.where(pair == 0, split[:, 1], split[:, 0]).astype(jnp.bfloat16)
    halves = mine + swapped(other, "pair").astype(jnp.float32)
    keep = jnp.where(far == 0, halves[0], halves[1])
    give = jnp.where(far == 0, halves[1], halves[0]).astype(jnp.bfloat16)
    projected = keep + swapped(give, "far").astype(jnp.float32)
    stream = (hidden_in.astype(jnp.float32) + projected).astype(jnp.bfloat16)
    stream = lax.optimization_barrier(stream)
    stream_wide = stream.astype(jnp.float32)
    inverse = lax.rsqrt(jnp.mean(stream_wide * stream_wide, axis=1, keepdims=True) + 1e-05)
    normed = (stream_wide * inverse * norm_gain).astype(jnp.bfloat16)
    experts = router_weight.shape[1]
    logits = jnp.dot(normed, router_weight, preferred_element_type=jnp.float32)
    ids = jnp.arange(experts, dtype=jnp.int32)
    chosen = jnp.any(expert_ids[:, :, None] == ids[None, None, :], axis=1)
    raised_gates = jnp.where(chosen, jnp.exp(logits), 0.0)
    gates = raised_gates / jnp.sum(raised_gates, axis=1, keepdims=True)
    coarse = gates.astype(jnp.bfloat16)
    fine = (gates - coarse.astype(jnp.float32)).astype(jnp.bfloat16)
    fill = -(model + 2 * experts) % 128
    blank = jnp.zeros((rows, fill), jnp.bfloat16)
    packet = jnp.concatenate([normed, coarse, fine, blank], axis=1)
    everyone = gather_rows(packet)
    count = everyone.shape[0]
    everyone = everyone.reshape(count * rows, model + 2 * experts + fill)
    tokens = everyone[:, :model]
    tails = everyone[:, model : model + 2 * experts].astype(jnp.float32)
    own = lax.axis_index("seq")
    here = jnp.arange(2 * experts, dtype=jnp.int32) % experts == own
    weight = jnp.sum(jnp.where(here[None, :], tails, 0.0), axis=1, keepdims=True)
    total = 0.0
    for gate_part, up_part, down_part in zip(gates_w, ups_w, downs_w):
        total = total + down_piece(swiglu_piece(tokens, gate_part, up_part), down_part)
    answer = (total * weight).astype(jnp.bfloat16)
    expert_sum = scatter_rows(answer.reshape(count, rows, model))
    return (stream_wide + expert_sum).astype(jnp.bfloat16)


def mapped(body, mesh, fsdp):
    every = ("seq", *fsdp)
    return jax.shard_map(
        body,
        mesh=mesh,
        in_specs=(
            P("seq", fsdp),
            P("seq", fsdp),
            P(every, None),
            P(fsdp, None),
            P(),
            P(),
            P(every, None),
            P("seq", None, fsdp),
            P("seq", None, fsdp),
            P("seq", None, fsdp),
        ),
        out_specs=P(every, None),
        check_vma=False,
    )


def solution(mesh):
    owners = mesh.shape["seq"]

    def run(*args):
        experts = args[5].shape[1]
        if experts == owners and owners == 2 * TOPK and mesh.shape["fsdp"] == 4:
            cut = Mesh(mesh.devices.reshape(owners, 2, 2), ("seq", "far", "pair"))
            return mapped(dense_device, cut, ("far", "pair"))(*args)
        return mapped(per_device, mesh, ("fsdp",))(*args)

    return run
```
